32 devices in a mesh: section: 4 (over y, x), dev: 8 (over z, core).
Axes of the slice: x: 2, y: 2, z: 4, core: 2. Of those that a mesh axis runs over, the one named last changes fastest.
Arguments:
- patches: bfloat16 [4, 12288, 1280], P('section', 'dev'), may hold values from -6 to 6
- win_count: int32 [4, 8], P('section'), may hold values from 1 to 24, 64 in all within a row
- dest_perm: int32 [4, 8], P('section'), may hold values from 0 to 7, each once within a row
- win_groups: int32 [4, 8, 24], P('section'), may hold values from 2 to 16
- norm_gain: float32 [1280], replicated, may hold values from 0.5 to 1.5
- qkv_weight: bfloat16 [1280, 3840], P('dev')
- qkv_bias: float32 [3840], replicated, may hold values from -1.5 to 1.5
- proj_weight: bfloat16 [1280, 1280], P('dev'), may hold values from -0.15625 to 0.15625
- proj_bias: float32 [1280], replicated, may hold values from -1.5 to 1.5
- merge_gain: float32 [1280], replicated, may hold values from 0.5 to 1.5
- owner: int32 [4, 1024, 1], P('section', 'dev'), may hold values from 0 to 3; in each aligned block of 128 rows (0 to 127, 128 to 255, ..., all dimensions but the last counted through in order) at most 64 rows name the same one
Outputs:
- dispatched: bfloat16 [4, 2048, 5120], P('section', 'dev')
The draws below stay inside these ranges and needn't reach their ends.
Inputs may be any that keep to these rules, and one draw needn't show every extreme that they name: `win_count`: within each section's row the counts sum to 8 times the devices of dev, and the largest is 24. `dest_perm`: each section's row is a permutation. `win_groups`: entries of slots past a device's count are not read. Among the 128 rows of one device, at most 64 have the same owner, and some device of every draw reaches 64.
All inputs are finite; a program needn't handle non-finite values.
Results may differ from the reference program's by a relative error of at most 0.0051.
Values may be sent and summed in bfloat16 or wider, within the bound.
A program may use at most 128 MiB of HBM per device.

```python
import math
import jax
import jax.numpy as jnp
import numpy as np
from jax import lax

D = 1280
HEADS = 16
HEAD_DIM = 80
WIN = 64
DST_WIN = 8
SRC_WIN = 24
MERGED = 128
CAP = 64
N_SECTION = 4
N_DEV = 8


def draw_qkv_weight(key, part):
    first = jax.random.fold_in(jax.random.fold_in(key, 11), 0)
    base = jax.random.normal(first, (D, 3 * D), jnp.float32) * D ** (-0.5)
    return base.astype(jnp.bfloat16)


def place_ends(array, rng, smallest, top_value):
    longest = array.shape.index(max(array.shape))
    spots = []
    for shift in (0, 1):
        where = [jax.random.randint(jax.random.fold_in(rng, axis), (), 0, length) for axis, length in enumerate(array.shape)]
        where[longest] = (where[longest] + shift) % array.shape[longest]
        spots.append(tuple(where))
    return array.at[spots[0]].set(smallest).at[spots[1]].set(top_value)


def block_levels(rng, dims, pieces, low, top_value):
    def one(position, parts):
        draws = jax.random.uniform(jax.random.fold_in(jax.random.fold_in(rng, 6), position), (parts,), jnp.float32, low / len(pieces), top_value / len(pieces))
        return jnp.repeat(jnp.exp(draws), dims[position] // parts).reshape((-1,) + (1,) * (len(dims) - position - 1))

    loudness = one(*pieces[0])
    for cut in pieces[1:]:
        loudness = loudness * one(*cut)
    return loudness


def profile(amount, total, most, lean):
    weights = [(1 << 20) // math.isqrt(rank ** lean) + 1 for rank in range(2, amount + 1)]
    surplus, given = total - most - (amount - 1), [1] * (amount - 1)
    while surplus > 0:
        free = [i for i in range(amount - 1) if given[i] < most]
        pool, budget = sum([weights[i] for i in free]), surplus
        for i in free:
            addition = min(most - given[i], max(1, budget * weights[i] // pool), surplus)
            given[i] = given[i] + addition
            surplus = surplus - addition
    return np.array([most] + given)


def ragged(rng, number_of, total, reach, lean):
    if number_of == 2:
        one = jax.random.randint(rng, (), max(1, total - reach), min(reach, total - 1) + 1)
        return jnp.stack([one, total - one])
    sizes = jnp.asarray(profile(number_of, total, reach, lean), jnp.int32)
    pairs = (number_of - 1) // 2
    donor, taker = sizes[1:1 + 2 * pairs:2], sizes[2:2 + 2 * pairs:2]
    room = jnp.minimum(donor - 1, reach - taker)
    passed = jax.random.randint(jax.random.fold_in(rng, 1), (pairs,), 0, 1 << 20) % (room + 1)
    sizes = sizes.at[1:1 + 2 * pairs:2].set(donor - passed).at[2:2 + 2 * pairs:2].set(taker + passed)
    return sizes[jax.random.permutation(jax.random.fold_in(rng, 2), number_of)]


def shared_out(rng, own, number, rows, count, top, limit, lean):
    sequence = jax.random.permutation(rng, count)
    packed, common = portions_of(count, rows * top, limit, lean, True), portions_of(count, rows * top, limit, lean, False)
    places = jnp.arange(count)

    def named(lengths, offset_by):
        used = int((lengths > 0).sum())
        fixed = max(1, used // 4)
        passed = fixed + (places - fixed + offset_by * (used - fixed)) % max(1, count - fixed)
        return jnp.zeros((count,), jnp.int32).at[sequence[jnp.where(places < fixed, places, passed)]].set(jnp.asarray(lengths, jnp.int32))

    lengths = jnp.where(number % 4 == 0, named(packed, number // 4), named(common, number - number // 4 - 1))
    mixed = jax.random.permutation(jax.random.fold_in(own, 3), count)
    donor, sink = mixed[0:count // 2 * 2:2], mixed[1:count // 2 * 2:2]
    room = jnp.minimum(lengths[donor] - 1, limit - lengths[sink]) // 2
    room = jnp.where((donor == sequence[0]) | (sink == sequence[0]) | (lengths[sink] == 0), 0, jnp.maximum(room, 0))
    passed = jax.random.randint(jax.random.fold_in(own, 4), (count // 2,), 0, 1 << 20) % (room + 1)
    lengths = lengths.at[donor].add(-passed).at[sink].add(passed)
    items = jnp.searchsorted(jnp.cumsum(lengths), jnp.arange(rows * top), side="right").astype(jnp.int32)
    listing = items.reshape(top, rows).T
    listing = listing[jax.random.permutation(jax.random.fold_in(own, 1), rows)]
    offset_by = jax.random.randint(jax.random.fold_in(own, 2), (rows, 1), 0, top)
    return jnp.take_along_axis(listing, (jnp.arange(top)[None, :] + offset_by) % top, axis=1)


def portions_of(count, total, most, skew, full):
    weights = [(1 << 20) // math.isqrt(grade ** skew) + 1 for grade in range(1, count + 1)]
    largest = most if full else min(most, max(-(-total // count), total * weights[0] // sum(weights)))
    least = 1 if total - largest >= count - 1 else 0
    holding, spare = [largest] + [least] * (count - 1), total - largest - least * (count - 1)
    while spare > 0:
        movable = [i for i in range(1, count) if holding[i] < largest] or [i for i in range(1, count) if holding[i] < most]
        mass, left = sum([weights[i] for i in movable]), spare
        for i in movable:
            more = min(most - holding[i], max(1, left * weights[i] // mass), spare)
            holding[i] = holding[i] + more
            spare = spare - more
    return np.array(holding)


def normal_values(own_key, dims, deviation, reach, pieces=(), kind=jnp.bfloat16):
    values = deviation * jax.random.normal(own_key, dims, jnp.float32)
    if pieces:
        values = values * block_levels(own_key, dims, pieces, -0.22, 0.18)
    return jnp.clip(values, -reach, reach).astype(kind)


def setup_inputs(seed: int = 0) -> dict:
    key_list = jax.random.split(jax.random.key(seed), 12)
    patches = normal_values(key_list[0], (N_SECTION, N_DEV * SRC_WIN * WIN, D), 1.0, 6.0, ((0, 4), (1, 8)))
    win_count = jax.vmap(lambda own: ragged(own, N_DEV, DST_WIN * N_DEV, SRC_WIN, 2))(jax.random.split(key_list[1], N_SECTION)).reshape((N_SECTION, N_DEV)).astype(jnp.int32)
    dest_perm = jax.vmap(lambda own: jax.random.permutation(own, N_DEV))(jax.random.split(key_list[2], N_SECTION)).reshape((N_SECTION, N_DEV)).astype(jnp.int32)
    win_groups = place_ends(jax.random.randint(key_list[3], (N_SECTION, N_DEV, SRC_WIN), 2, WIN // 4 + 1), jax.random.fold_in(key_list[3], 1), 2, (WIN // 4 + 1) - 1).astype(jnp.int32)
    norm_gain = jnp.clip(1.0 + 0.1 * jax.random.normal(key_list[4], (D,), jnp.float32), 0.5, 1.5)
    qkv_weight = draw_qkv_weight(jax.random.fold_in(key_list[11], 71), 0)
    qkv_bias = normal_values(key_list[6], (3 * D,), 0.3, 1.5, (), jnp.float32)
    proj_weight = normal_values(key_list[7], (D, D), D ** -0.5, 0.15625, ((0, 8),))
    proj_bias = normal_values(key_list[8], (D,), 0.3, 1.5, (), jnp.float32)
    merge_gain = jnp.clip(1.0 + 0.1 * jax.random.normal(key_list[9], (D,), jnp.float32), 0.5, 1.5)
    owner_keys = jax.random.split(jax.random.fold_in(key_list[10], 1), N_SECTION * (N_DEV * MERGED) // MERGED)
    owner_turns = jax.random.permutation(jax.random.fold_in(key_list[10], 3), N_SECTION * (N_DEV * MERGED) // MERGED)
    owner = jax.vmap(lambda own, number: shared_out(jax.random.fold_in(key_list[10], 2), own, number, MERGED, N_SECTION, 1, CAP, 2))(owner_keys, owner_turns).reshape((N_SECTION, N_DEV * MERGED, 1))
    return {"patches": patches, "win_count": win_count, "dest_perm": dest_perm, "win_groups": win_groups, "norm_gain": norm_gain, "qkv_weight": qkv_weight, "qkv_bias": qkv_bias, "proj_weight": proj_weight, "proj_bias": proj_bias, "merge_gain": merge_gain, "owner": owner}


def normalize(values, gain):
    return values * lax.rsqrt(lax.optimization_barrier(jnp.mean(values * values, axis=-1, keepdims=True)) + 1e-06) * gain

def encode(windows, groups, norm_gain, qkv_weight, qkv_bias, proj_weight, proj_bias, merge_gain):
    count = windows.shape[0]
    values = windows.reshape(count * WIN, D).astype(jnp.float32)
    normed = normalize(values, norm_gain).astype(jnp.bfloat16)
    triple = (jnp.dot(normed, qkv_weight, preferred_element_type=jnp.float32) + qkv_bias).astype(jnp.bfloat16)
    triple = triple.reshape(count, WIN, 3, HEADS, HEAD_DIM).astype(jnp.float32)
    scores = jnp.einsum('bqhe,bkhe->bhqk', triple[:, :, 0], triple[:, :, 1]) * HEAD_DIM ** (-0.5)
    living = jnp.arange(WIN, dtype=jnp.int32)[None, :] < 4 * groups[:, None]
    scores = jnp.where(living[:, None, None, :], scores, -1e+30)
    highest = lax.optimization_barrier(jnp.max(scores, axis=-1, keepdims=True))
    powers = jnp.exp(scores - highest)
    probs = (powers / lax.optimization_barrier(jnp.sum(powers, axis=-1, keepdims=True))).astype(jnp.bfloat16)
    mixed = jnp.einsum('bhqk,bkhe->bqhe', probs.astype(jnp.float32), triple[:, :, 2]).astype(jnp.bfloat16)
    mixed = mixed.reshape(count * WIN, D)
    encoded = values + jnp.dot(mixed, proj_weight, preferred_element_type=jnp.float32) + proj_bias
    final = normalize(encoded, merge_gain) * living.reshape(count * WIN, 1).astype(jnp.float32)
    return final.reshape(count * WIN // 4, 4 * D).astype(jnp.bfloat16)

def pack(merged, owners):
    sections = jnp.arange(N_SECTION, dtype=jnp.int32)
    hits = (owners[:, None] == sections[None, :]).astype(jnp.int32)
    ranks = lax.optimization_barrier(jnp.sum((jnp.cumsum(hits, axis=0) - hits) * hits, axis=1)).astype(jnp.int32)
    places = (owners * CAP + ranks).astype(jnp.int32)
    chosen = places[None, :] == jnp.arange(N_SECTION * CAP, dtype=jnp.int32)[:, None]
    ladder = jnp.arange(merged.shape[0], dtype=jnp.int32)
    indices = lax.optimization_barrier(jnp.sum(chosen.astype(jnp.int32) * ladder[None, :], axis=1)).astype(jnp.int32)
    filled = jnp.any(chosen, axis=1)
    return jnp.where(filled[:, None], merged[indices], jnp.zeros((), merged.dtype))

def reference(patches, win_count, dest_perm, win_groups, norm_gain, qkv_weight, qkv_bias, proj_weight, proj_bias, merge_gain, owner):
    buffers = []
    ladder = jnp.arange(N_DEV, dtype=jnp.int32)
    for section in range(N_SECTION):
        source_windows = patches[section].reshape(N_DEV, SRC_WIN, WIN, D)
        counts = win_count[section]
        before = lax.optimization_barrier(jnp.sum(jnp.where(ladder[None, :] < ladder[:, None], counts[None, :], 0), axis=1)).astype(jnp.int32)
        inverse = lax.optimization_barrier(jnp.sum(ladder[:, None] * (dest_perm[section][:, None] == ladder[None, :]).astype(jnp.int32), axis=0)).astype(jnp.int32)
        groups_table = win_groups[section]
        owner_table = owner[section, :, 0].reshape(N_DEV, MERGED)

        def one_device(target):
            wanted = (jnp.arange(DST_WIN, dtype=jnp.int32) * N_DEV + inverse[target]).astype(jnp.int32)
            source = (lax.optimization_barrier(jnp.sum((before[None, :] <= wanted[:, None]).astype(jnp.int32), axis=1)) - 1).astype(jnp.int32)
            within = (wanted - before[source]).astype(jnp.int32)
            merged = encode(source_windows[source, within], groups_table[source, within], norm_gain, qkv_weight, qkv_bias, proj_weight, proj_bias, merge_gain)
            return pack(merged, owner_table[target])
        buffers.append(lax.map(one_device, ladder))
    stacked = jnp.stack(buffers).reshape(N_SECTION, N_DEV, N_SECTION, CAP, 4 * D)
    return stacked.transpose(2, 1, 0, 3, 4).reshape(N_SECTION, N_DEV * N_SECTION * CAP, 4 * D)
```

```python
import functools

import jax
import jax.numpy as jnp
from jax import lax
from jax.experimental import pallas as pl
from jax.experimental.pallas import tpu as pltpu
from jax.sharding import PartitionSpec as P

D = 1280
HEADS = 16
HEAD_DIM = D // HEADS
WIN = 64
DST_WIN = 8
SRC_WIN = 24
PAIR = 2 * WIN
CHUNK = 768


def whole_weight(shard):
    section_count = lax.axis_size("section")
    dev_count = lax.axis_size("dev")
    sub_rows = shard.shape[0] // section_count
    portion = lax.dynamic_slice_in_dim(shard, lax.axis_index("section") * sub_rows, sub_rows, 0)
    gathered = lax.all_gather(portion, ("section", "dev"), axis=0, tiled=True)
    return (
        gathered.reshape(section_count, dev_count, sub_rows, shard.shape[1])
        .transpose(1, 0, 2, 3)
        .reshape(section_count * dev_count * sub_rows, shard.shape[1])
    )


def normalize(values, gain):
    return values * lax.rsqrt(jnp.mean(values * values, axis=-1, keepdims=True) + 1e-06) * gain


def encode_kernel(
    steps, x_ref, gain_ref, w_ref, wb_ref, pw_ref, pb_ref, mg_ref, row_ref, key_ref, pick_ref,
    out_ref, normed, qkv, mixed, enc, tall, merged,
):
    step = pl.program_id(0)
    rows = x_ref.shape[0]

    @pl.when(step == 0)
    def _():
        @pl.loop(0, rows // WIN)
        def _(i):
            at = pl.ds(pl.multiple_of(i * WIN, WIN), WIN)
            normed[at, :] = normalize(x_ref[at, :].astype(jnp.float32), gain_ref[...]).astype(jnp.bfloat16)

    cols = pl.ds(pl.multiple_of(step * CHUNK, CHUNK), CHUNK)
    qkv[:, cols] = (
        jnp.dot(normed[...], w_ref[...], preferred_element_type=jnp.float32) + wb_ref[...]
    ).astype(jnp.bfloat16)

    @pl.when(step == steps - 1)
    def _():
        same = (
            lax.broadcasted_iota(jnp.int32, (PAIR, PAIR), 0) // WIN
            == lax.broadcasted_iota(jnp.int32, (PAIR, PAIR), 1) // WIN
        )

        @pl.loop(0, rows // PAIR)
        def _(pair):
            at = pl.ds(pl.multiple_of(pair * PAIR, PAIR), PAIR)
            valid = same & (key_ref[pair] > 0.5)
            blocks = [None] * (D // 128)
            for h in range(HEADS):
                low, high = h * HEAD_DIM, (h + 1) * HEAD_DIM
                begin, end = low // 128 * 128, -(-high // 128) * 128
                lane = lax.broadcasted_iota(jnp.int32, (1, end - begin), 1) + begin
                inside = ((lane >= low) & (lane < high)).astype(jnp.bfloat16)
                q = qkv[at, begin:end] * inside
                k = qkv[at, D + begin:D + end]
                v = qkv[at, 2 * D + begin:2 * D + end] * inside
                scores = lax.dot_general(
                    q, k, (((1,), (1,)), ((), ())), preferred_element_type=jnp.float32
                ) * HEAD_DIM ** (-0.5)
                scores = jnp.where(valid, scores, -1e30)
                powers = jnp.exp(scores - jnp.max(scores, axis=-1, keepdims=True))
                probs = (powers / jnp.sum(powers, axis=-1, keepdims=True)).astype(jnp.bfloat16)
                o = jnp.dot(probs, v, preferred_element_type=jnp.float32)
                for b in range(begin // 128, end // 128):
                    piece = o[:, b * 128 - begin:(b + 1) * 128 - begin]
                    blocks[b] = piece if blocks[b] is None else blocks[b] + piece
            for b in range(D // 128):
                mixed[at, b * 128:(b + 1) * 128] = blocks[b].astype(jnp.bfloat16)

        enc[...] = jnp.dot(mixed[...], pw_ref[...], preferred_element_type=jnp.float32)

        @pl.loop(0, rows // WIN)
        def _(i):
            at = pl.ds(pl.multiple_of(i * WIN, WIN), WIN)
            encoded = x_ref[at, :].astype(jnp.float32) + enc[at, :] + pb_ref[...]
            final = normalize(encoded, mg_ref[...]) * row_ref[at, :]
            for b in range(D // 128):
                tall[b, at, :] = final[:, b * 128:(b + 1) * 128]

        count = rows // 4
        for j in range(4):
            for b in range(D // 128):
                merged[:, j * D + b * 128:j * D + (b + 1) * 128] = tall[
                    b, pl.ds(j, count, stride=4), :
                ].astype(jnp.bfloat16)

        @pl.loop(0, 4)
        def _(j):
            at = pl.ds(pl.multiple_of(j * D, D), D)
            out_ref[:, at] = jnp.dot(
                pick_ref[...], merged[:, at], preferred_element_type=jnp.float32
            ).astype(jnp.bfloat16)


def encode(x, row_live, key_live, pick, norm_gain, qkv_w, qkv_bias, proj_w, proj_bias, merge_gain):
    rows = x.shape[0]
    steps = 3 * D // CHUNK
    slots = pick.shape[0]

    def full(*shape):
        return pl.BlockSpec(shape, lambda i: (0,) * len(shape))

    return pl.pallas_call(
        functools.partial(encode_kernel, steps),
        grid=(steps,),
        in_specs=[
            full(rows, D),
            full(1, D),
            pl.BlockSpec((D, CHUNK), lambda i: (0, i)),
            pl.BlockSpec((1, CHUNK), lambda i: (0, i)),
            full(D, D),
            full(1, D),
            full(1, D),
            full(rows, 1),
            full(rows // PAIR, 1, PAIR),
            full(slots, rows // 4),
        ],
        out_specs=full(slots, 4 * D),
        out_shape=jax.ShapeDtypeStruct((slots, 4 * D), jnp.bfloat16),
        scratch_shapes=[
            pltpu.VMEM((rows, D), jnp.bfloat16),
            pltpu.VMEM((rows, 3 * D), jnp.bfloat16),
            pltpu.VMEM((rows, D), jnp.bfloat16),
            pltpu.VMEM((rows, D), jnp.float32),
            pltpu.VMEM((D // 128, rows, 128), jnp.float32),
            pltpu.VMEM((rows // 4, 4 * D), jnp.bfloat16),
        ],
        compiler_params=pltpu.CompilerParams(
            dimension_semantics=("arbitrary",), vmem_limit_bytes=56 * 1024 * 1024
        ),
        cost_estimate=pl.CostEstimate(
            flops=2 * rows * D * 4 * D, bytes_accessed=8 * D * D + 6 * rows * D, transcendentals=0
        ),
    )(
        x, norm_gain[None], qkv_w, qkv_bias[None], proj_w, proj_bias[None], merge_gain[None],
        row_live, key_live, pick,
    )


def picking(owners, section_count, capacity):
    sections = jnp.arange(section_count, dtype=jnp.int32)
    hits = (owners[:, None] == sections[None, :]).astype(jnp.int32)
    ranks = jnp.sum((jnp.cumsum(hits, axis=0) - hits) * hits, axis=1)
    places = owners * capacity + ranks
    return places[None, :] == jnp.arange(section_count * capacity, dtype=jnp.int32)[:, None]


def body(
    patches,
    win_count,
    dest_perm,
    win_groups,
    norm_gain,
    qkv_weight,
    qkv_bias,
    proj_weight,
    proj_bias,
    merge_gain,
    owner,
):
    dev_count = lax.axis_size("dev")
    section_count = lax.axis_size("section")
    position = lax.axis_index("dev")
    windows = patches.reshape(SRC_WIN, WIN, D)
    counts = win_count[0]
    ladder = jnp.arange(dev_count, dtype=jnp.int32)
    before = jnp.sum(jnp.where(ladder[None, :] < ladder[:, None], counts[None, :], 0), axis=1)
    inverse = jnp.sum(
        ladder[:, None] * (dest_perm[0][:, None] == ladder[None, :]).astype(jnp.int32), axis=0
    )
    pair_slots = (SRC_WIN + dev_count - 1) // dev_count
    residue = jnp.mod(inverse - before[position], dev_count)
    picked = jnp.arange(pair_slots, dtype=jnp.int32)[None, :] * dev_count + residue[:, None]
    outgoing = windows[jnp.minimum(picked, SRC_WIN - 1)].reshape(dev_count * pair_slots * WIN, D)
    arrived = lax.all_to_all(outgoing, "dev", split_axis=0, concat_axis=0, tiled=True).reshape(
        dev_count * pair_slots, WIN, D
    )
    wanted = jnp.arange(DST_WIN, dtype=jnp.int32) * dev_count + inverse[position]
    source = jnp.sum((before[None, :] <= wanted[:, None]).astype(jnp.int32), axis=1) - 1
    within = wanted - before[source]
    balanced = arrived[source * pair_slots + within // dev_count].reshape(DST_WIN * WIN, D)
    groups = win_groups[0][source, within]
    living = (jnp.arange(WIN, dtype=jnp.int32)[None, :] < 4 * groups[:, None]).astype(jnp.float32)

    merged_rows = DST_WIN * WIN // 4
    capacity = 2 * merged_rows // section_count
    pick = picking(owner[0, :, 0], section_count, capacity).astype(jnp.bfloat16)
    packed = encode(
        balanced,
        living.reshape(DST_WIN * WIN, 1),
        living.reshape(DST_WIN * WIN // PAIR, 1, PAIR),
        pick,
        norm_gain,
        whole_weight(qkv_weight),
        qkv_bias,
        whole_weight(proj_weight),
        proj_bias,
        merge_gain,
    )
    delivered = lax.all_to_all(packed, "section", split_axis=0, concat_axis=0, tiled=True)
    return delivered.reshape(1, section_count * capacity, 4 * D)


def solution(mesh):
    return jax.shard_map(
        body,
        mesh=mesh,
        in_specs=(
            P("section", "dev", None),
            P("section", None),
            P("section", None),
            P("section", None, None),
            P(),
            P("dev", None),
            P(),
            P("dev", None),
            P(),
            P(),
            P("section", "dev", None),
        ),
        out_specs=P("section", "dev", None),
        check_vma=False,
    )
```

```python
import functools

import jax
import jax.numpy as jnp
from jax import lax
from jax.experimental import pallas as pl
from jax.experimental.pallas import tpu as pltpu
from jax.sharding import PartitionSpec as P

D = 1280
HEADS = 16
HEAD_DIM = D // HEADS
WIN = 64
DST_WIN = 8
SRC_WIN = 24
PAIR = 2 * WIN
CHUNK = 768


def whole_weight(shard):
    section_count = lax.axis_size("section")
    dev_count = lax.axis_size("dev")
    sub_rows = shard.shape[0] // section_count
    portion = lax.dynamic_slice_in_dim(shard, lax.axis_index("section") * sub_rows, sub_rows, 0)
    gathered = lax.all_gather(portion, ("section", "dev"), axis=0, tiled=True)
    return (
        gathered.reshape(section_count, dev_count, sub_rows, shard.shape[1])
        .transpose(1, 0, 2, 3)
        .reshape(section_count * dev_count * sub_rows, shard.shape[1])
    )


def normalize(values, gain):
    return values * lax.rsqrt(jnp.mean(values * values, axis=-1, keepdims=True) + 1e-06) * gain


def encode_kernel(
    steps, x_ref, gain_ref, w_ref, wb_ref, pw_ref, pb_ref, mg_ref, row_ref, key_ref, pick_ref,
    out_ref, normed, qkv, mixed, enc, tall, merged,
):
    step = pl.program_id(0)
    rows = x_ref.shape[0]

    @pl.when(step == 0)
    def _():
        @pl.loop(0, rows // WIN)
        def _(i):
            at = pl.ds(pl.multiple_of(i * WIN, WIN), WIN)
            normed[at, :] = normalize(x_ref[at, :].astype(jnp.float32), gain_ref[...]).astype(jnp.bfloat16)

    cols = pl.ds(pl.multiple_of(step * CHUNK, CHUNK), CHUNK)
    qkv[:, cols] = (
        jnp.dot(normed[...], w_ref[...], preferred_element_type=jnp.float32) + wb_ref[...]
    ).astype(jnp.bfloat16)

    @pl.when(step == steps - 1)
    def _():
        same = (
            lax.broadcasted_iota(jnp.int32, (PAIR, PAIR), 0) // WIN
            == lax.broadcasted_iota(jnp.int32, (PAIR, PAIR), 1) // WIN
        )

        @pl.loop(0, rows // PAIR)
        def _(pair):
            at = pl.ds(pl.multiple_of(pair * PAIR, PAIR), PAIR)
            valid = same & (key_ref[pair] > 0.5)
            blocks = [None] * (D // 128)
            for h in range(HEADS):
                low, high = h * HEAD_DIM, (h + 1) * HEAD_DIM
                begin, end = low // 128 * 128, -(-high // 128) * 128
                lane = lax.broadcasted_iota(jnp.int32, (1, end - begin), 1) + begin
                inside = ((lane >= low) & (lane < high)).astype(jnp.bfloat16)
                q = qkv[at, begin:end] * inside
                k = qkv[at, D + begin:D + end]
                v = qkv[at, 2 * D + begin:2 * D + end] * inside
                scores = lax.dot_general(
                    q, k, (((1,), (1,)), ((), ())), preferred_element_type=jnp.float32
                ) * HEAD_DIM ** (-0.5)
                scores = jnp.where(valid, scores, -1e30)
                powers = jnp.exp(scores - jnp.max(scores, axis=-1, keepdims=True))
                probs = (powers / jnp.sum(powers, axis=-1, keepdims=True)).astype(jnp.bfloat16)
                o = jnp.dot(probs, v, preferred_element_type=jnp.float32)
                for b in range(begin // 128, end // 128):
                    piece = o[:, b * 128 - begin:(b + 1) * 128 - begin]
                    blocks[b] = piece if blocks[b] is None else blocks[b] + piece
            for b in range(D // 128):
                mixed[at, b * 128:(b + 1) * 128] = blocks[b].astype(jnp.bfloat16)

        enc[...] = jnp.dot(mixed[...], pw_ref[...], preferred_element_type=jnp.float32)

        @pl.loop(0, rows // WIN)
        def _(i):
            at = pl.ds(pl.multiple_of(i * WIN, WIN), WIN)
            encoded = x_ref[at, :].astype(jnp.float32) + enc[at, :] + pb_ref[...]
            final = normalize(encoded, mg_ref[...]) * row_ref[at, :]
            for b in range(D // 128):
                tall[b, at, :] = final[:, b * 128:(b + 1) * 128]

        count = rows // 4
        for j in range(4):
            for b in range(D // 128):
                merged[:, j * D + b * 128:j * D + (b + 1) * 128] = tall[
                    b, pl.ds(j, count, stride=4), :
                ].astype(jnp.bfloat16)

        @pl.loop(0, 4)
        def _(j):
            at = pl.ds(pl.multiple_of(j * D, D), D)
            out_ref[:, at] = jnp.dot(
                pick_ref[...], merged[:, at], preferred_element_type=jnp.float32
            ).astype(jnp.bfloat16)


def encode(x, row_live, key_live, pick, norm_gain, weights, qkv_bias, proj_bias, merge_gain):
    rows = x.shape[0]
    steps = 3 * D // CHUNK
    slots = pick.shape[0]

    def full(*shape):
        return pl.BlockSpec(shape, lambda i: (0,) * len(shape))

    return pl.pallas_call(
        functools.partial(encode_kernel, steps),
        grid=(steps,),
        in_specs=[
            full(rows, D),
            full(1, D),
            pl.BlockSpec((D, CHUNK), lambda i: (0, i)),
            pl.BlockSpec((1, CHUNK), lambda i: (0, i)),
            pl.BlockSpec((D, D), lambda i: (0, 3)),
            full(1, D),
            full(1, D),
            full(rows, 1),
            full(rows // PAIR, 1, PAIR),
            full(slots, rows // 4),
        ],
        out_specs=full(slots, 4 * D),
        out_shape=jax.ShapeDtypeStruct((slots, 4 * D), jnp.bfloat16),
        scratch_shapes=[
            pltpu.VMEM((rows, D), jnp.bfloat16),
            pltpu.VMEM((rows, 3 * D), jnp.bfloat16),
            pltpu.VMEM((rows, D), jnp.bfloat16),
            pltpu.VMEM((rows, D), jnp.float32),
            pltpu.VMEM((D // 128, rows, 128), jnp.float32),
            pltpu.VMEM((rows // 4, 4 * D), jnp.bfloat16),
        ],
        compiler_params=pltpu.CompilerParams(
            dimension_semantics=("arbitrary",), vmem_limit_bytes=56 * 1024 * 1024
        ),
        cost_estimate=pl.CostEstimate(
            flops=2 * rows * D * 4 * D, bytes_accessed=8 * D * D + 6 * rows * D, transcendentals=0
        ),
    )(
        x, norm_gain[None], weights, qkv_bias[None], weights, proj_bias[None], merge_gain[None],
        row_live, key_live, pick,
    )


def picking(owners, section_count, capacity):
    sections = jnp.arange(section_count, dtype=jnp.int32)
    hits = (owners[:, None] == sections[None, :]).astype(jnp.int32)
    ranks = jnp.sum((jnp.cumsum(hits, axis=0) - hits) * hits, axis=1)
    places = owners * capacity + ranks
    return places[None, :] == jnp.arange(section_count * capacity, dtype=jnp.int32)[:, None]


def body(
    patches,
    win_count,
    dest_perm,
    win_groups,
    norm_gain,
    qkv_weight,
    qkv_bias,
    proj_weight,
    proj_bias,
    merge_gain,
    owner,
):
    dev_count = lax.axis_size("dev")
    section_count = lax.axis_size("section")
    position = lax.axis_index("dev")
    windows = patches.reshape(SRC_WIN, WIN, D)
    counts = win_count[0]
    ladder = jnp.arange(dev_count, dtype=jnp.int32)
    before = jnp.sum(jnp.where(ladder[None, :] < ladder[:, None], counts[None, :], 0), axis=1)
    inverse = jnp.sum(
        ladder[:, None] * (dest_perm[0][:, None] == ladder[None, :]).astype(jnp.int32), axis=0
    )
    pair_slots = (SRC_WIN + dev_count - 1) // dev_count
    residue = jnp.mod(inverse - before[position], dev_count)
    picked = jnp.arange(pair_slots, dtype=jnp.int32)[None, :] * dev_count + residue[:, None]
    outgoing = windows[jnp.minimum(picked, SRC_WIN - 1)].reshape(dev_count * pair_slots * WIN, D)
    arrived = lax.all_to_all(outgoing, "dev", split_axis=0, concat_axis=0, tiled=True).reshape(
        dev_count * pair_slots, WIN, D
    )
    wanted = jnp.arange(DST_WIN, dtype=jnp.int32) * dev_count + inverse[position]
    source = jnp.sum((before[None, :] <= wanted[:, None]).astype(jnp.int32), axis=1) - 1
    within = wanted - before[source]
    balanced = arrived[source * pair_slots + within // dev_count].reshape(DST_WIN * WIN, D)
    groups = win_groups[0][source, within]
    living = (jnp.arange(WIN, dtype=jnp.int32)[None, :] < 4 * groups[:, None]).astype(jnp.float32)

    merged_rows = DST_WIN * WIN // 4
    capacity = 2 * merged_rows // section_count
    pick = picking(owner[0, :, 0], section_count, capacity).astype(jnp.bfloat16)
    packed = encode(
        balanced,
        living.reshape(DST_WIN * WIN, 1),
        living.reshape(DST_WIN * WIN // PAIR, 1, PAIR),
        pick,
        norm_gain,
        whole_weight(jnp.concatenate([qkv_weight, proj_weight], axis=1)),
        qkv_bias,
        proj_bias,
        merge_gain,
    )
    delivered = lax.all_to_all(packed, "section", split_axis=0, concat_axis=0, tiled=True)
    return delivered.reshape(1, section_count * capacity, 4 * D)


def solution(mesh):
    return jax.shard_map(
        body,
        mesh=mesh,
        in_specs=(
            P("section", "dev", None),
            P("section", None),
            P("section", None),
            P("section", None, None),
            P(),
            P("dev", None),
            P(),
            P("dev", None),
            P(),
            P(),
            P("section", "dev", None),
        ),
        out_specs=P("section", "dev", None),
        check_vma=False,
    )
```
